256 devices in a mesh: group: 4 (over x_hi, core), seq: 64 (over x_lo, y, z).
Axes of the slice: x: 4 (x_hi: 2, x_lo: 2; x = x_hi * 2 + x_lo), y: 4, z: 8, core: 2. Of those that a mesh axis runs over, the one named last changes fastest.
Arguments:
- prefill_query: bfloat16 [4, 4096, 8192], P('group', 'seq'), may hold values from -40 to 40
- prefill_key: bfloat16 [4, 4096, 1024], P('group', 'seq'), may hold values from -40 to 40
- prefill_value: bfloat16 [4, 4096, 1024], P('group', 'seq'), may hold values from -6 to 6
- lengths: int32 [4], replicated, may hold values from 1024 to 4096
- verify_query: bfloat16 [512, 4, 8192], P(('group', 'seq')), may hold values from -40 to 40
- verify_key: bfloat16 [512, 4, 1024], P(('group', 'seq')), may hold values from -6 to 6
- verify_value: bfloat16 [512, 4, 1024], P(('group', 'seq')), may hold values from -6 to 6
- owner: int32 [512], replicated, may hold values from 0 to 3
- cached: int32 [512], replicated, may hold values from 1 to 64
Outputs:
- prefill_out: bfloat16 [4, 4096, 8192], P('group', 'seq')
- verify_out: bfloat16 [512, 4, 8192], P(('group', 'seq'))
The draws below stay inside these ranges and needn't reach their ends.
All inputs are finite; a program needn't handle non-finite values.
Results may differ from the reference program's by a relative error of at most 0.005.
Values may be sent and summed in bfloat16 or wider, within the bound.
No kernel may reach another device: no remote copies, remote signals or barrier semaphores. Data moves between devices by JAX's collectives and lax.ppermute only.
A program may use at most 192 MiB of HBM per device.

```python
import math
import jax
import jax.numpy as jnp
from jax import lax

HQ = 64
HK = 8
HD = 128
STEPS = 4
BLK = 64
TOK_DEV = 64
TRAJ = 4
LENGTH = 4096
ROWS = 512
N_GROUP = 4
N_SEQ = 64


def draw_prefill_query(key, part):
    values = jax.random.truncated_normal(jax.random.fold_in(key, 21), -6.0, 6.0, (TRAJ, LENGTH, HQ * HD), jnp.float32)
    return values.astype(jnp.bfloat16)


def draw_prefill_key(key, part):
    values = jax.random.truncated_normal(jax.random.fold_in(key, 22), -6.0, 6.0, (TRAJ, LENGTH, HK * HD), jnp.float32)
    return values.astype(jnp.bfloat16)


def draw_verify_query(key, part):
    values = jax.random.truncated_normal(jax.random.fold_in(key, 24), -6.0, 6.0, (ROWS, STEPS, HQ * HD), jnp.float32)
    return values.astype(jnp.bfloat16)


def touch_ends(values, key, smallest, top_value):
    longest = values.shape.index(max(values.shape))
    spots = []
    for shift in (0, 1):
        where = [jax.random.randint(jax.random.fold_in(key, axis), (), 0, length) for axis, length in enumerate(values.shape)]
        where[longest] = (where[longest] + shift) % values.shape[longest]
        spots.append(tuple(where))
    return values.at[spots[0]].set(smallest).at[spots[1]].set(top_value)


def block_scale(own_key, shape, cuts, least, top_value):
    def one(axis_at, blocks):
        heights = jax.random.uniform(jax.random.fold_in(jax.random.fold_in(own_key, 6), axis_at), (blocks,), jnp.float32, least / len(cuts), top_value / len(cuts))
        return jnp.repeat(jnp.exp(heights), shape[axis_at] // blocks).reshape((-1,) + (1,) * (len(shape) - axis_at - 1))

    factor_of = one(*cuts[0])
    for cut in cuts[1:]:
        factor_of = factor_of * one(*cut)
    return factor_of


def scatter_about(key, dims, scale, reach, shards=(), kind=jnp.bfloat16):
    entries = jax.random.normal(key, dims, jnp.float32) * scale
    if len(shards) > 0:
        entries = block_scale(key, dims, shards, -0.22, 0.18) * entries
    return jnp.clip(entries, min=-reach, max=reach).astype(kind)


def setup_inputs(seed: int = 0) -> dict:
    splits = jax.random.split(jax.random.key(seed), 10)
    return {
        "prefill_query": draw_prefill_query(jax.random.fold_in(splits[9], 71), 0),
        "prefill_key": draw_prefill_key(jax.random.fold_in(splits[9], 71), 0),
        "prefill_value": scatter_about(splits[2], (TRAJ, LENGTH, HK * HD), 1.0, 6.0, ((0, 4), (1, 64))),
        "lengths": touch_ends(jax.random.randint(splits[3], (TRAJ,), TOK_DEV * N_SEQ // 4, TOK_DEV * N_SEQ + 1), jax.random.fold_in(splits[3], 1), TOK_DEV * N_SEQ // 4, TOK_DEV * N_SEQ).astype(jnp.int32),
        "verify_query": draw_verify_query(jax.random.fold_in(splits[9], 71), 0),
        "verify_key": scatter_about(splits[5], (ROWS, STEPS, HK * HD), 1.0, 6.0, ((0, 256),)),
        "verify_value": scatter_about(splits[6], (ROWS, STEPS, HK * HD), 1.0, 6.0, ((0, 256),)),
        "owner": touch_ends(jax.random.randint(splits[7], (ROWS,), 0, N_GROUP), jax.random.fold_in(splits[7], 1), 0, N_GROUP - 1).astype(jnp.int32),
        "cached": touch_ends(jax.random.randint(splits[8], (ROWS,), 1, TOK_DEV * N_SEQ // BLK + 1), jax.random.fold_in(splits[8], 1), 1, (TOK_DEV * N_SEQ // BLK + 1) - 1).astype(jnp.int32),
    }


def prefill_part(query_one, key_one, value_one, length):
    block = math.gcd(LENGTH, 256)
    group = HQ // HK
    scale = HD ** -0.5
    keys = key_one.reshape(LENGTH, HK, HD).astype(jnp.float32)
    values = value_one.reshape(LENGTH, HK, HD).astype(jnp.float32)
    queries = query_one.reshape(LENGTH // block, block, HK, group, HD)
    starts = jnp.arange(LENGTH // block, dtype=jnp.int32) * block

    def one_block(inputs):
        query_block, start = inputs
        scores = jnp.einsum("tkgd,jkd->tkgj", query_block.astype(jnp.float32), keys) * scale
        slots = start + jnp.arange(block, dtype=jnp.int32)
        columns = jnp.arange(LENGTH, dtype=jnp.int32)
        allowed = (columns[None, :] <= slots[:, None]) & (columns[None, :] < length)
        allowed = allowed[:, None, None, :]
        masked = jnp.where(allowed, scores, -1e30)
        highest = jnp.max(masked, axis=-1, keepdims=True)
        weights = jnp.where(allowed, jnp.exp(scores - highest), 0.0)
        summed = jnp.sum(weights, axis=-1)
        rounded = lax.optimization_barrier(weights.astype(jnp.bfloat16))
        mixed = jnp.einsum("tkgj,jkd->tkgd", rounded.astype(jnp.float32), values)
        return (mixed / summed[..., None]).astype(jnp.bfloat16).reshape(block, HQ * HD)

    return lax.map(one_block, (queries, starts)).reshape(LENGTH, HQ * HD)


def reference(prefill_query, prefill_key, prefill_value, lengths, verify_query, verify_key, verify_value, owner, cached):
    prefill_out = lax.map(lambda inputs: prefill_part(*inputs), (prefill_query, prefill_key, prefill_value, lengths))
    group = HQ // HK
    scale = HD ** -0.5
    row_block = math.gcd(ROWS, 8)
    blocks = ROWS // row_block
    queries = verify_query.reshape(blocks, row_block, STEPS, HK, group, HD)
    fresh_keys = verify_key.reshape(blocks, row_block, STEPS, HK, HD)
    fresh_values = verify_value.reshape(blocks, row_block, STEPS, HK, HD)
    limits = jnp.minimum(cached * BLK, lengths[owner]).astype(jnp.int32).reshape(blocks, row_block)
    owners = owner.reshape(blocks, row_block)
    cache_keys = prefill_key.reshape(TRAJ, LENGTH, HK, HD)
    cache_values = prefill_value.reshape(TRAJ, LENGTH, HK, HD)
    steps_order = jnp.arange(STEPS, dtype=jnp.int32)
    causal = (steps_order[None, :] <= steps_order[:, None])[None, :, None, None, :]

    def one_block(inputs):
        query_block, key_block, value_block, owner_block, limit_block = inputs
        row_keys = cache_keys[owner_block].astype(jnp.float32)
        row_values = cache_values[owner_block].astype(jnp.float32)
        query_wide = query_block.astype(jnp.float32)
        scores = jnp.einsum("rtkgd,rjkd->rtkgj", query_wide, row_keys) * scale
        columns = jnp.arange(LENGTH, dtype=jnp.int32)
        allowed = (columns[None, :] < limit_block[:, None])[:, None, None, None, :]
        fresh = jnp.einsum("rtkgd,rskd->rtkgs", query_wide, key_block.astype(jnp.float32)) * scale
        highest = jnp.maximum(jnp.max(jnp.where(allowed, scores, -1e30), axis=-1), jnp.max(jnp.where(causal, fresh, -1e30), axis=-1))
        weights = jnp.where(allowed, jnp.exp(scores - highest[..., None]), 0.0)
        fresh_weights = jnp.where(causal, jnp.exp(fresh - highest[..., None]), 0.0)
        summed = jnp.sum(weights, axis=-1) + jnp.sum(fresh_weights, axis=-1)
        rounded = lax.optimization_barrier(weights.astype(jnp.bfloat16))
        fresh_rounded = lax.optimization_barrier(fresh_weights.astype(jnp.bfloat16))
        mixed = jnp.einsum("rtkgj,rjkd->rtkgd", rounded.astype(jnp.float32), row_values)
        mixed = mixed + jnp.einsum("rtkgs,rskd->rtkgd", fresh_rounded.astype(jnp.float32), value_block.astype(jnp.float32))
        return (mixed / summed[..., None]).astype(jnp.bfloat16).reshape(row_block, STEPS, HQ * HD)

    verify_out = lax.map(one_block, (queries, fresh_keys, fresh_values, owners, limits)).reshape(ROWS, STEPS, HQ * HD)
    return prefill_out, verify_out
```

```python
import jax
import jax.numpy as jnp
from jax import lax
from jax.experimental import pallas as pl
from jax.experimental.pallas import tpu as pltpu
from jax.sharding import Mesh
from jax.sharding import PartitionSpec as P

HQ = 64
HK = 8
HD = 128
BLK = 64
QH = HQ // HK
HEAD_W = QH * HD
FRESH_W = HEAD_W + 2 * HD
XY = ("x", "y")
GXY = ("g", "x", "y")
NEG = -1e30
LOG2E = 1.4426950408889634
COEF = HD ** (-0.5) * LOG2E


def dot_nt(a, b):
    return lax.dot_general(a, b, (((1,), (1,)), ((), ())), preferred_element_type=jnp.float32)


def dot_nn(a, b):
    return lax.dot_general(a, b, (((1,), (0,)), ((), ())), preferred_element_type=jnp.float32)


def lane_groups(x):
    return [x[:, k * 128 : (k + 1) * 128] for k in range(x.shape[1] // 128)]


def fold(op, x):
    parts = lane_groups(x)
    while len(parts) > 1:
        parts = [op(parts[k], parts[k + 1]) for k in range(0, len(parts) - 1, 2)] + (
            [parts[-1]] if len(parts) % 2 else []
        )
    return parts[0]


def softmax_step(s, m_old, l_old, acc_old, v):
    rows = s.shape[0]
    top = jnp.max(fold(jnp.maximum, s), axis=1, keepdims=True)
    if m_old is None:
        m_new = jnp.broadcast_to(top, (rows, 128))
    else:
        m_new = jnp.maximum(m_old, top)
    w = jnp.concatenate([jnp.exp2(part - m_new) for part in lane_groups(s)], axis=1)
    l_new = fold(jnp.add, w)
    mixed = dot_nn(w.astype(jnp.bfloat16), v)
    if m_old is not None:
        factor = jnp.exp2(m_old - m_new)
        l_new = l_old * factor + l_new
        mixed = acc_old * factor + mixed
    return m_new, l_new, mixed


def prefill_kernel(info, q_ref, kv_ref, o_ref, q_s, m_s, l_s, acc_s):
    p = pl.program_id(0)
    z = info[0]
    length = info[1]
    tok = q_ref.shape[1]
    zs = kv_ref.shape[0]
    width = zs * tok
    rows = QH * tok
    for h in range(QH):
        q_s[h * tok : (h + 1) * tok, :] = q_ref[0, :, h * HD : (h + 1) * HD]
    m_s[...] = jnp.full((rows, 128), NEG, jnp.float32)
    l_s[...] = jnp.zeros((rows, 128), jnp.float32)
    acc_s[...] = jnp.zeros((rows, HD), jnp.float32)
    half = rows // 2

    def chunk(j, masked):
        kv = kv_ref[:, j, :, :].reshape(width, 2 * HD)
        k = kv[:, :HD]
        v = kv[:, HD:]
        for part in range(2):
            at = slice(part * half, (part + 1) * half)
            s = dot_nt(q_s[at, :], k) * COEF
            if masked:
                col = lax.broadcasted_iota(jnp.int32, (half, width), 1) + j * width
                row = lax.broadcasted_iota(jnp.int32, (half, width), 0) % tok
                slot = p * width + z * tok + row
                s = jnp.where((col <= slot) & (col < length), s, NEG)
            m, l, acc = softmax_step(s, m_s[at, :], l_s[at, :], acc_s[at, :], v)
            m_s[at, :] = m
            l_s[at, :] = l
            acc_s[at, :] = acc

    full = jnp.minimum(p, length // width)

    def body(j, carry):
        chunk(j, False)
        return carry

    lax.fori_loop(0, full, body, 0)
    chunk(full, True)
    out = acc_s[...] / jnp.sum(l_s[...], axis=1, keepdims=True)
    out = out.astype(o_ref.dtype)
    for h in range(QH):
        o_ref[0, :, h * HD : (h + 1) * HD] = out[h * tok : (h + 1) * tok, :]


def prefill(info, q, kv):
    n, tok, _ = q.shape
    zs = kv.shape[0]
    rows = QH * tok
    return pl.pallas_call(
        prefill_kernel,
        out_shape=jax.ShapeDtypeStruct(q.shape, q.dtype),
        grid_spec=pltpu.PrefetchScalarGridSpec(
            num_scalar_prefetch=1,
            grid=(n,),
            in_specs=[
                pl.BlockSpec((1, tok, HEAD_W), lambda p, info: (p, 0, 0)),
                pl.BlockSpec((zs, n, tok, 2 * HD), lambda p, info: (0, 0, 0, 0)),
            ],
            out_specs=pl.BlockSpec((1, tok, HEAD_W), lambda p, info: (p, 0, 0)),
            scratch_shapes=[
                pltpu.VMEM((rows, HD), jnp.bfloat16),
                pltpu.VMEM((rows, 128), jnp.float32),
                pltpu.VMEM((rows, 128), jnp.float32),
                pltpu.VMEM((rows, HD), jnp.float32),
            ],
        ),
        compiler_params=pltpu.CompilerParams(vmem_limit_bytes=40 * 2**20),
        cost_estimate=pl.CostEstimate(
            flops=20 * 10**9, transcendentals=10**7, bytes_accessed=4 * 2**20
        ),
        name="prefill",
    )(info, q, kv)


def verify_kernel(info, x_ref, pos_row, lim_row, pos_col, kv_ref, o_ref, x_s, lim_s, o_s):
    n_batch = info[0]
    cells = pos_row.shape[1]
    zs, ps, tok, _ = kv_ref.shape
    width = zs * tok
    steps = 4
    cut = 8 * steps
    pick = lax.broadcasted_iota(jnp.int32, (cells, cells), 0) == pos_row[...]
    x = x_ref[...].reshape(cells, FRESH_W)
    x_s[...] = dot_nn(pick.astype(jnp.bfloat16), x).astype(jnp.bfloat16)
    limits = jnp.sum(jnp.where(pick, lim_row[...], 0.0), axis=1, keepdims=True)
    lim_s[...] = jnp.broadcast_to(limits, (cells, 128))
    o_s[...] = jnp.zeros((cells, HEAD_W), jnp.bfloat16)

    def batch(b, carry):
        at = pl.ds(pl.multiple_of(b * cut, cut), cut)
        q = jnp.concatenate([x_s[at, h * HD : (h + 1) * HD] for h in range(QH)], axis=0)
        lim = jnp.concatenate([lim_s[at, :]] * QH, axis=0)
        near = pl.ds(pl.multiple_of((b // 4) * 128, 128), 128)
        fk = x_s[near, HEAD_W : HEAD_W + HD]
        fv = x_s[near, HEAD_W + HD :]
        rows = QH * cut
        col = lax.broadcasted_iota(jnp.int32, (rows, 128), 1) - (b % 4) * cut
        row = lax.broadcasted_iota(jnp.int32, (rows, 128), 0) % cut
        seen = (col <= row) & (col >= row - row % steps)
        s = jnp.where(seen, dot_nt(q, fk) * COEF, NEG)
        state = softmax_step(s, None, None, None, fv)
        lane = lax.broadcasted_iota(jnp.int32, (rows, 128), 1).astype(jnp.float32)

        def chunk(j, state):
            kv = kv_ref[:, j, :, :].reshape(width, 2 * HD)
            s = dot_nt(q, kv[:, :HD]) * COEF
            left = lim - (j * width).astype(jnp.float32)
            s = jnp.concatenate(
                [
                    jnp.where(lane + 128.0 * k < left, part, NEG)
                    for k, part in enumerate(lane_groups(s))
                ],
                axis=1,
            )
            return softmax_step(s, *state, kv[:, HD:])

        count = (info[1 + b] + width - 1) // width
        m, l, acc = lax.fori_loop(0, count, chunk, state)
        out = (acc / jnp.sum(l, axis=1, keepdims=True)).astype(jnp.bfloat16)
        for h in range(QH):
            o_s[at, h * HD : (h + 1) * HD] = out[h * cut : (h + 1) * cut, :]
        return carry

    lax.fori_loop(0, n_batch, batch, 0)
    place = lax.broadcasted_iota(jnp.int32, (cells, cells), 1) == pos_col[...]
    out = dot_nn(place.astype(jnp.bfloat16), o_s[...]).astype(jnp.bfloat16)
    o_ref[...] = out.reshape(o_ref.shape)


def verify(info, x, pos_row, lim_row, pos_col, kv):
    cells = pos_row.shape[1]
    full = lambda a: pl.BlockSpec(a.shape, lambda i, info, n=a.ndim: (0,) * n)
    out = jax.ShapeDtypeStruct((*x.shape[:2], HEAD_W), x.dtype)
    return pl.pallas_call(
        verify_kernel,
        out_shape=out,
        grid_spec=pltpu.PrefetchScalarGridSpec(
            num_scalar_prefetch=1,
            grid=(1,),
            in_specs=[full(a) for a in (x, pos_row, lim_row, pos_col, kv)],
            out_specs=pl.BlockSpec(out.shape, lambda i, info: (0, 0, 0)),
            scratch_shapes=[
                pltpu.VMEM((cells, FRESH_W), jnp.bfloat16),
                pltpu.VMEM((cells, 128), jnp.float32),
                pltpu.VMEM((cells, HEAD_W), jnp.bfloat16),
            ],
        ),
        compiler_params=pltpu.CompilerParams(vmem_limit_bytes=40 * 2**20),
        cost_estimate=pl.CostEstimate(
            flops=4 * 10**9, transcendentals=10**6, bytes_accessed=4 * 2**20
        ),
        name="verify",
    )(info, x, pos_row, lim_row, pos_col, kv)


def pack_kv_kernel(k_ref, v_ref, o_ref):
    for h in range(HK):
        o_ref[h, :, :HD] = k_ref[0, :, h * HD : (h + 1) * HD]
        o_ref[h, :, HD:] = v_ref[0, :, h * HD : (h + 1) * HD]


def pack_kv(k, v):
    tok = k.shape[1]
    return pl.pallas_call(
        pack_kv_kernel,
        out_shape=jax.ShapeDtypeStruct((HK, tok, 2 * HD), k.dtype),
        name="pack_kv",
    )(k, v)


def move_kernel(x_ref, o_ref):
    o_ref[...] = x_ref[...].reshape(o_ref.shape)


def pack_q(q):
    tok = q.shape[1]
    return pl.pallas_call(
        move_kernel,
        out_shape=jax.ShapeDtypeStruct((HK, tok, HEAD_W), q.dtype),
        grid=(HK,),
        in_specs=[pl.BlockSpec((1, tok, HEAD_W), lambda p: (0, 0, p))],
        out_specs=pl.BlockSpec((1, tok, HEAD_W), lambda p: (p, 0, 0)),
        name="pack_q",
    )(q)


def unpack_o(o):
    tok = o.shape[1]
    return pl.pallas_call(
        move_kernel,
        out_shape=jax.ShapeDtypeStruct((1, tok, HK * HEAD_W), o.dtype),
        grid=(HK,),
        in_specs=[pl.BlockSpec((1, tok, HEAD_W), lambda p: (p, 0, 0))],
        out_specs=pl.BlockSpec((1, tok, HEAD_W), lambda p: (0, 0, p)),
        name="unpack_o",
    )(o)


def pack_rows_kernel(q_ref, k_ref, v_ref, o_ref):
    groups = o_ref.shape[0] // HK

    def joined(ref, at):
        return jnp.concatenate(
            [ref[i, :, at].astype(jnp.float32) for i in range(ref.shape[0])], axis=0
        ).astype(o_ref.dtype)

    for h in range(HK):
        q = joined(q_ref, slice(h * HEAD_W, (h + 1) * HEAD_W))
        k = joined(k_ref, slice(h * HD, (h + 1) * HD))
        v = joined(v_ref, slice(h * HD, (h + 1) * HD))
        for g in range(groups):
            o_ref[g * HK + h, :, :HEAD_W] = q
            o_ref[g * HK + h, :, HEAD_W : HEAD_W + HD] = k
            o_ref[g * HK + h, :, HEAD_W + HD :] = v


def pack_rows(q, k, v, groups):
    return pl.pallas_call(
        pack_rows_kernel,
        out_shape=jax.ShapeDtypeStruct((groups * HK, q.shape[0] * q.shape[1], FRESH_W), q.dtype),
        name="pack_rows",
    )(q, k, v)


def sum_rows_kernel(x_ref, o_ref):
    groups = x_ref.shape[0] // HK
    steps = o_ref.shape[1]
    for h in range(HK):
        total = x_ref[h].astype(jnp.float32)
        for g in range(1, groups):
            total = total + x_ref[g * HK + h].astype(jnp.float32)
        for i in range(o_ref.shape[0]):
            o_ref[i, :, h * HEAD_W : (h + 1) * HEAD_W] = total[
                i * steps : (i + 1) * steps, :
            ].astype(o_ref.dtype)


def sum_rows(x, rows, steps):
    return pl.pallas_call(
        sum_rows_kernel,
        out_shape=jax.ShapeDtypeStruct((rows, steps, HK * HEAD_W), x.dtype),
        name="sum_rows",
    )(x)


def tables(owner, cached, length, g, z, groups, per, zs, rows, steps):
    own = lax.dynamic_index_in_dim(owner.reshape(groups, per, zs, rows), z, 2, False).reshape(-1)
    held = lax.dynamic_index_in_dim(cached.reshape(groups, per, zs, rows), z, 2, False).reshape(-1)
    limit = jnp.where(own == g, jnp.minimum(held * BLK, length), 0)
    n = limit.shape[0]
    index = jnp.arange(n, dtype=jnp.int32)
    ahead = (limit[None, :] > limit[:, None]) | (
        (limit[None, :] == limit[:, None]) & (index[None, :] < index[:, None])
    )
    rank = jnp.sum(ahead.astype(jnp.int32), axis=1)
    pos = (rank[:, None] * steps + jnp.arange(steps, dtype=jnp.int32)[None, :]).reshape(-1)
    mine = jnp.repeat(limit > 0, steps)
    firsts = jnp.arange(n // 8, dtype=jnp.int32) * 8
    tops = jnp.sum(jnp.where(rank[None, :] == firsts[:, None], limit[None, :], 0), axis=1)
    n_batch = jnp.sum((tops > 0).astype(jnp.int32))
    info = jnp.concatenate([n_batch[None], tops])
    pos_row = pos[None, :]
    lim_row = jnp.repeat(limit, steps).astype(jnp.float32)[None, :]
    pos_col = jnp.where(mine, pos, -1)[:, None]
    return info, pos_row, lim_row, pos_col


def per_device(
    prefill_query,
    prefill_key,
    prefill_value,
    lengths,
    verify_query,
    verify_key,
    verify_value,
    owner,
    cached,
):
    groups = lax.axis_size("g")
    zs = lax.axis_size("z")
    per = lax.axis_size(XY)
    g = lax.axis_index("g")
    z = lax.axis_index("z")
    rows, steps, _ = verify_query.shape
    length = jnp.sum(jnp.where(jnp.arange(groups, dtype=jnp.int32) == g, lengths, 0))

    kv = lax.all_to_all(pack_kv(prefill_key, prefill_value), XY, 0, 0, tiled=True)
    kv_all = lax.all_gather(kv, "z", axis=0, tiled=False)

    q_in, x_in, _ = lax.optimization_barrier(
        (
            pack_q(prefill_query),
            pack_rows(verify_query, verify_key, verify_value, groups),
            kv,
        )
    )
    x = lax.all_to_all(x_in, GXY, 0, 0, tiled=True)
    q = lax.all_to_all(q_in, XY, 0, 0, tiled=True)

    info, pos_row, lim_row, pos_col = tables(
        owner, cached, length, g, z, groups, per, zs, rows, steps
    )
    decoded = verify(info, x, pos_row, lim_row, pos_col, kv_all)
    returned = lax.all_to_all(decoded, GXY, 0, 0, tiled=True)
    out = prefill(jnp.stack([z, length]).astype(jnp.int32), q, kv_all)
    out = lax.all_to_all(out, XY, 0, 0, tiled=True)
    return unpack_o(out), sum_rows(returned, rows, steps)


def solution(mesh):
    split = Mesh(mesh.devices.reshape(4, 2, 4, 8), ("g", "x", "y", "z"))
    token = P("g", ("x", "y", "z"), None)
    row = P(("g", "x", "y", "z"), None, None)
    return jax.shard_map(
        per_device,
        mesh=split,
        in_specs=(token, token, token, P(), row, row, row, P(), P()),
        out_specs=(token, row),
        check_vma=False,
    )
```

```python
import functools

import jax
import jax.numpy as jnp
from jax import lax
from jax.experimental import pallas as pl
from jax.experimental.pallas import tpu as pltpu
from jax.sharding import Mesh
from jax.sharding import PartitionSpec as P

HQ = 64
HK = 8
HD = 128
BLK = 64
N_Z = 8
STEPS = 4
BATCH = 16
QH = HQ // HK
HEAD_W = QH * HD
FRESH_W = HEAD_W + 2 * HD
XY = ("x", "y")
GXY = ("g", "x", "y")
NEG = -1e30
LOG2E = 1.4426950408889634
COEF = HD ** (-0.5) * LOG2E


def dot_nt(a, b):
    return lax.dot_general(a, b, (((1,), (1,)), ((), ())), preferred_element_type=jnp.float32)


def dot_nn(a, b):
    return lax.dot_general(a, b, (((1,), (0,)), ((), ())), preferred_element_type=jnp.float32)


def lane_groups(x):
    return [x[:, k * 128 : (k + 1) * 128] for k in range(x.shape[1] // 128)]


def fold(op, x):
    parts = lane_groups(x)
    while len(parts) > 1:
        parts = [op(parts[k], parts[k + 1]) for k in range(0, len(parts) - 1, 2)] + (
            [parts[-1]] if len(parts) % 2 else []
        )
    return parts[0]


def split_scaled(q):
    x = q.astype(jnp.float32) * COEF
    high = x.astype(jnp.bfloat16)
    return jnp.concatenate([high, (x - high.astype(jnp.float32)).astype(jnp.bfloat16)], axis=1)


def score(q2, k):
    return dot_nt(q2, jnp.concatenate([k, k], axis=1))


def softmax_step(s, m_old, acc_old, v):
    top = jnp.max(fold(jnp.maximum, s), axis=1, keepdims=True)
    m_new = jnp.broadcast_to(top, (s.shape[0], 128)) if m_old is None else jnp.maximum(m_old, top)
    w = jnp.concatenate([jnp.exp2(part - m_new) for part in lane_groups(s)], axis=1)
    mixed = dot_nn(w.astype(jnp.bfloat16), jnp.concatenate([v, jnp.ones_like(v)], axis=1))
    if m_old is not None:
        factor = jnp.exp2(m_old - m_new)
        mixed = acc_old * jnp.concatenate([factor, factor], axis=1) + mixed
    return m_new, mixed


def key_slots(segments, z, zs, tok, span):
    width = sum(n for _, _, n in segments)
    col = lax.broadcasted_iota(jnp.int32, (1, span * width), 1)
    at = jnp.zeros((1, span * width), jnp.int32)
    off = 0
    for block in range(span):
        for shift, start, n in segments:
            base = ((z - shift) & (zs - 1)) * tok + block * zs * tok + start - off
            at = jnp.where((col >= off) & (col < off + n), col + base, at)
            off += n
    return at


def joined_blocks(refs, j, span, part):
    return jnp.concatenate([ref[j + i, :, part] for i in range(span) for ref in refs], axis=0)


KEYS = slice(0, HD)
VALUES = slice(HD, 2 * HD)


def prefill_kernel(segments, info, q_ref, *refs):
    n = len(segments)
    kv_refs = refs[:n]
    o_ref, q_s, m_s, acc_s, sa, sb = refs[n:]
    z = info[0]
    length = info[1]
    count, tok, _ = q_ref.shape
    rows = QH * tok
    block = N_Z * tok
    edge = length // block

    def split(p):
        for h in range(QH):
            q_s[p, h * tok : (h + 1) * tok, :] = split_scaled(q_ref[p, :, h * HD : (h + 1) * HD])

    def fill(s_ref, p, j):
        s_ref[...] = score(q_s[p], joined_blocks(kv_refs, j, 1, KEYS))

    def begin(s_ref, p):
        j = jnp.minimum(p, edge)
        at = key_slots(segments, z, N_Z, tok, 1) + j * block
        row = lax.broadcasted_iota(jnp.int32, (rows, 1), 0) % tok
        end = jnp.minimum(p * block + z * tok + row, length - 1)
        s = jnp.where(at <= end, s_ref[...], NEG)
        v = joined_blocks(kv_refs, j, 1, VALUES)
        m_s[p], acc_s[p] = softmax_step(s, None, None, v)

    def take(s_ref, p, j):
        v = joined_blocks(kv_refs, j, 1, VALUES)
        m_s[p], acc_s[p] = softmax_step(s_ref[...], m_s[p], acc_s[p], v)

    def item(t):
        return info[2 + 2 * t], info[3 + 2 * t]

    split(0)
    fill(sa, 0, 0)

    def edges(i, carry):
        p = 2 * i
        split(p + 1)
        fill(sb, p + 1, jnp.minimum(p + 1, edge))
        begin(sa, p)
        split(p + 2)
        fill(sa, p + 2, jnp.minimum(p + 2, edge))
        begin(sb, p + 1)
        return carry

    lax.fori_loop(0, count // 2 - 1, edges, 0)
    split(count - 1)
    fill(sb, count - 1, jnp.minimum(count - 1, edge))
    begin(sa, count - 2)
    fill(sa, *item(0))
    begin(sb, count - 1)

    def body(i, carry):
        fill(sb, *item(2 * i + 1))
        take(sa, *item(2 * i))
        fill(sa, *item(2 * i + 2))
        take(sb, *item(2 * i + 1))
        return carry

    cols = jnp.minimum(edge, count - 1)
    items = (count - 1) * cols - cols * (cols - 1) // 2
    lax.fori_loop(0, items // 2, body, 0)

    @pl.when(items % 2 == 1)
    def _():
        take(sa, *item(items - 1))

    def finish(p, carry):
        out = (acc_s[p, :, :HD] / acc_s[p, :, HD:]).astype(o_ref.dtype)
        for h in range(QH):
            o_ref[p, :, h * HD : (h + 1) * HD] = out[h * tok : (h + 1) * tok, :]
        return carry

    lax.fori_loop(0, count, finish, 0)


def open_items(count):
    pairs = [(p, j) for j in range(count - 1) for p in range(j + 1, count)] + [(1, 0)] * 2
    return [k for pair in pairs for k in pair]


def whole(shape):
    return pl.BlockSpec(shape, lambda i, info: (0,) * len(shape))


def prefill(info, q, kvs, segments):
    n, tok, _ = q.shape
    rows = QH * tok
    return pl.pallas_call(
        functools.partial(prefill_kernel, tuple(segments)),
        out_shape=jax.ShapeDtypeStruct(q.shape, q.dtype),
        grid_spec=pltpu.PrefetchScalarGridSpec(
            num_scalar_prefetch=1,
            grid=(1,),
            in_specs=[whole(a.shape) for a in (q, *kvs)],
            out_specs=whole(q.shape),
            scratch_shapes=[
                pltpu.VMEM((n, rows, 2 * HD), jnp.bfloat16),
                pltpu.VMEM((n, rows, 128), jnp.float32),
                pltpu.VMEM((n, rows, 2 * HD), jnp.float32),
                pltpu.VMEM((rows, N_Z * tok), jnp.float32),
                pltpu.VMEM((rows, N_Z * tok), jnp.float32),
            ],
        ),
        compiler_params=pltpu.CompilerParams(vmem_limit_bytes=40 * 2**20),
        cost_estimate=pl.CostEstimate(
            flops=20 * 10**9, transcendentals=10**7, bytes_accessed=4 * 2**20
        ),
        name="prefill",
    )(info, q, *kvs)


def verify_kernel(segments, info, x_ref, pos_row, lim_row, pos_col, *refs):
    n = len(segments)
    kv_refs = refs[:n]
    o_ref, x_s, lim_s, o_s, q_s, m_s, acc_s, sa, sb = refs[n:]
    z = info[0]
    n_batch = info[1]
    cells = pos_row.shape[1]
    blocks, tok, _ = kv_refs[0].shape
    width = N_Z * tok
    cut = BATCH * STEPS
    rows = QH * cut
    pick = lax.broadcasted_iota(jnp.int32, (cells, cells), 0) == pos_row[...]
    x = x_ref[...].reshape(cells, FRESH_W)
    x_s[...] = dot_nn(pick.astype(jnp.bfloat16), x).astype(jnp.bfloat16)
    limits = jnp.sum(jnp.where(pick, lim_row[...], 0.0), axis=1, keepdims=True)
    lim_s[...] = jnp.broadcast_to(limits, (cells, 128))
    o_s[...] = jnp.zeros((cells, HEAD_W), jnp.bfloat16)
    places = lane_groups(key_slots(segments, z, N_Z, tok, 1).astype(jnp.float32))

    def batch(b, carry):
        at = pl.ds(pl.multiple_of(b * cut, cut), cut)
        for h in range(QH):
            q_s[h * cut : (h + 1) * cut, :] = split_scaled(x_s[at, h * HD : (h + 1) * HD])
        near = pl.ds(pl.multiple_of(b * cut // 128 * 128, 128), 128)
        col = lax.broadcasted_iota(jnp.int32, (1, 128), 1) - b * cut % 128
        row = lax.broadcasted_iota(jnp.int32, (rows, 1), 0) % cut
        seen = (col <= row) & (col >= row - row % STEPS)
        s = jnp.where(seen, score(q_s[...], x_s[near, HEAD_W : HEAD_W + HD]), NEG)
        m_s[...], acc_s[...] = softmax_step(s, None, None, x_s[near, HEAD_W + HD :])

        def fill(s_ref, j):
            k = joined_blocks(kv_refs, jnp.minimum(j, blocks - 1), 1, KEYS)
            s_ref[...] = score(q_s[...], k)

        def take(s_ref, j):
            left = jnp.concatenate([lim_s[at, :]] * QH, axis=0)
            left = left - (j * width).astype(jnp.float32)
            parts = [
                jnp.where(place < left, part, NEG)
                for place, part in zip(places, lane_groups(s_ref[...]))
            ]
            s = jnp.concatenate(parts, axis=1)
            v = joined_blocks(kv_refs, j, 1, VALUES)
            m_s[...], acc_s[...] = softmax_step(s, m_s[...], acc_s[...], v)

        count = (info[2 + b] + width - 1) // width
        fill(sa, 0)

        def body(i, carry):
            fill(sb, 2 * i + 1)
            take(sa, 2 * i)
            fill(sa, 2 * i + 2)
            take(sb, 2 * i + 1)
            return carry

        lax.fori_loop(0, count // 2, body, 0)

        @pl.when(count % 2 == 1)
        def _():
            take(sa, count - 1)

        out = (acc_s[:, :HD] / acc_s[:, HD:]).astype(jnp.bfloat16)
        for h in range(QH):
            o_s[at, h * HD : (h + 1) * HD] = out[h * cut : (h + 1) * cut, :]
        return carry

    lax.fori_loop(0, n_batch, batch, 0)
    place = lax.broadcasted_iota(jnp.int32, (cells, cells), 1) == pos_col[...]
    out = dot_nn(place.astype(jnp.bfloat16), o_s[...]).astype(jnp.bfloat16)
    o_ref[...] = out.reshape(o_ref.shape)


def verify(info, x, pos_row, lim_row, pos_col, kvs, segments):
    cells = pos_row.shape[1]
    rows = QH * BATCH * STEPS
    width = N_Z * kvs[0].shape[1]
    operands = (x, pos_row, lim_row, pos_col, *kvs)
    out = jax.ShapeDtypeStruct((*x.shape[:2], HEAD_W), x.dtype)
    return pl.pallas_call(
        functools.partial(verify_kernel, tuple(segments)),
        out_shape=out,
        grid_spec=pltpu.PrefetchScalarGridSpec(
            num_scalar_prefetch=1,
            grid=(1,),
            in_specs=[whole(a.shape) for a in operands],
            out_specs=whole(out.shape),
            scratch_shapes=[
                pltpu.VMEM((cells, FRESH_W), jnp.bfloat16),
                pltpu.VMEM((cells, 128), jnp.float32),
                pltpu.VMEM((cells, HEAD_W), jnp.bfloat16),
                pltpu.VMEM((rows, 2 * HD), jnp.bfloat16),
                pltpu.VMEM((rows, 128), jnp.float32),
                pltpu.VMEM((rows, 2 * HD), jnp.float32),
                pltpu.VMEM((rows, width), jnp.float32),
                pltpu.VMEM((rows, width), jnp.float32),
            ],
        ),
        compiler_params=pltpu.CompilerParams(vmem_limit_bytes=40 * 2**20),
        cost_estimate=pl.CostEstimate(
            flops=4 * 10**9, transcendentals=10**6, bytes_accessed=4 * 2**20
        ),
        name="verify",
    )(info, *operands)


def pack_kv_kernel(k_ref, v_ref, o_ref):
    for h in range(HK):
        o_ref[h, :, :HD] = k_ref[0, :, h * HD : (h + 1) * HD]
        o_ref[h, :, HD:] = v_ref[0, :, h * HD : (h + 1) * HD]


def pack_kv(k, v):
    tok = k.shape[1]
    return pl.pallas_call(
        pack_kv_kernel,
        out_shape=jax.ShapeDtypeStruct((HK, tok, 2 * HD), k.dtype),
        name="pack_kv",
    )(k, v)


def pack_q_kernel(x_ref, o_ref):
    for h in range(HK):
        o_ref[h] = x_ref[0, :, h * HEAD_W : (h + 1) * HEAD_W]


def pack_q(q):
    return pl.pallas_call(
        pack_q_kernel,
        out_shape=jax.ShapeDtypeStruct((HK, q.shape[1], HEAD_W), q.dtype),
        name="pack_q",
    )(q)


def unpack_o_kernel(x_ref, o_ref):
    for h in range(HK):
        o_ref[0, :, h * HEAD_W : (h + 1) * HEAD_W] = x_ref[h]


def unpack_o(o):
    return pl.pallas_call(
        unpack_o_kernel,
        out_shape=jax.ShapeDtypeStruct((1, o.shape[1], HK * HEAD_W), o.dtype),
        name="unpack_o",
    )(o)


def pack_rows_kernel(q_ref, k_ref, v_ref, o_ref):
    groups = o_ref.shape[0] // HK

    def joined(ref, at):
        return jnp.concatenate(
            [ref[i, :, at].astype(jnp.float32) for i in range(ref.shape[0])], axis=0
        ).astype(o_ref.dtype)

    for h in range(HK):
        q = joined(q_ref, slice(h * HEAD_W, (h + 1) * HEAD_W))
        k = joined(k_ref, slice(h * HD, (h + 1) * HD))
        v = joined(v_ref, slice(h * HD, (h + 1) * HD))
        for g in range(groups):
            o_ref[g * HK + h, :, :HEAD_W] = q
            o_ref[g * HK + h, :, HEAD_W : HEAD_W + HD] = k
            o_ref[g * HK + h, :, HEAD_W + HD :] = v


def pack_rows(q, k, v, groups):
    return pl.pallas_call(
        pack_rows_kernel,
        out_shape=jax.ShapeDtypeStruct((groups * HK, q.shape[0] * q.shape[1], FRESH_W), q.dtype),
        name="pack_rows",
    )(q, k, v)


def sum_rows_kernel(x_ref, o_ref):
    groups = x_ref.shape[0] // HK
    steps = o_ref.shape[1]
    for h in range(HK):
        total = x_ref[h].astype(jnp.float32)
        for g in range(1, groups):
            total = total + x_ref[g * HK + h].astype(jnp.float32)
        for i in range(o_ref.shape[0]):
            o_ref[i, :, h * HEAD_W : (h + 1) * HEAD_W] = total[
                i * steps : (i + 1) * steps, :
            ].astype(o_ref.dtype)


def sum_rows(x, rows, steps):
    return pl.pallas_call(
        sum_rows_kernel,
        out_shape=jax.ShapeDtypeStruct((rows, steps, HK * HEAD_W), x.dtype),
        name="sum_rows",
    )(x)


def tables(owner, cached, length, g, z, groups, per, zs, rows, steps):
    own = lax.dynamic_index_in_dim(owner.reshape(groups, per, zs, rows), z, 2, False).reshape(-1)
    held = lax.dynamic_index_in_dim(cached.reshape(groups, per, zs, rows), z, 2, False).reshape(-1)
    limit = jnp.where(own == g, jnp.minimum(held * BLK, length), 0)
    n = limit.shape[0]
    index = jnp.arange(n, dtype=jnp.int32)
    ahead = (limit[None, :] > limit[:, None]) | (
        (limit[None, :] == limit[:, None]) & (index[None, :] < index[:, None])
    )
    rank = jnp.sum(ahead.astype(jnp.int32), axis=1)
    pos = (rank[:, None] * steps + jnp.arange(steps, dtype=jnp.int32)[None, :]).reshape(-1)
    mine = jnp.repeat(limit > 0, steps)
    firsts = jnp.arange(n // BATCH, dtype=jnp.int32) * BATCH
    tops = jnp.sum(jnp.where(rank[None, :] == firsts[:, None], limit[None, :], 0), axis=1)
    n_batch = jnp.sum((tops > 0).astype(jnp.int32))
    info = jnp.concatenate([z[None], n_batch[None], tops]).astype(jnp.int32)
    pos_row = pos[None, :]
    lim_row = jnp.repeat(limit, steps).astype(jnp.float32)[None, :]
    pos_col = jnp.where(mine, pos, -1)[:, None]
    return info, pos_row, lim_row, pos_col


def per_device(
    prefill_query,
    prefill_key,
    prefill_value,
    lengths,
    verify_query,
    verify_key,
    verify_value,
    owner,
    cached,
):
    groups = lax.axis_size("g")
    zs = lax.axis_size("z")
    per = lax.axis_size(XY)
    g = lax.axis_index("g")
    z = lax.axis_index("z")
    rows, steps, _ = verify_query.shape
    tok = prefill_query.shape[1]
    half = tok // 2
    length = jnp.sum(jnp.where(jnp.arange(groups, dtype=jnp.int32) == g, lengths, 0))

    def along(array, shift):
        return lax.ppermute(array, "z", [(i, (i + shift) % zs) for i in range(zs)])

    def exchange(array, axes):
        return lax.all_to_all(array, axes, 0, 0, tiled=True)

    own = exchange(pack_kv(prefill_key, prefill_value), XY)
    q_in = pack_q(prefill_query)
    x_in = pack_rows(verify_query, verify_key, verify_value, groups)
    q = exchange(q_in, XY)
    up1, down1 = along(own, 1), along(own, -1)
    x = exchange(x_in, GXY)
    up2, down2 = along(up1, 1), along(down1, -1)
    up3, down3 = along(up2, 1), along(down2, -1)
    up4 = along(up2[:, :half], 2)
    down4 = along(down2[:, half:], -2)
    kvs = [own, up1, down1, up2, down2, up3, down3, up4, down4]
    segments = [(s, 0, tok) for s in (0, 1, -1, 2, -2, 3, -3)]
    segments += [(4, 0, half), (4, half, half)]

    where = jnp.concatenate(
        [jnp.stack([z, length]), jnp.array(open_items(per), dtype=jnp.int32)]
    ).astype(jnp.int32)
    info, pos_row, lim_row, pos_col = tables(
        owner, cached, length, g, z, groups, per, zs, rows, steps
    )
    decoded = verify(info, x, pos_row, lim_row, pos_col, kvs, segments)
    returned = exchange(decoded, GXY)
    out = prefill(where, q, kvs, segments)
    out = exchange(out, XY)
    return unpack_o(out), sum_rows(returned, rows, steps)


def solution(mesh):
    split = Mesh(mesh.devices.reshape(4, 2, 4, N_Z), ("g", "x", "y", "z"))
    token = P("g", ("x", "y", "z"), None)
    row = P(("g", "x", "y", "z"), None, None)
    return jax.shard_map(
        per_device,
        mesh=split,
        in_specs=(token, token, token, P(), row, row, row, P(), P()),
        out_specs=(token, row),
        check_vma=False,
    )
```

```python
import functools

import jax
import jax.numpy as jnp
from jax import lax
from jax.experimental import pallas as pl
from jax.experimental.pallas import tpu as pltpu
from jax.sharding import Mesh
from jax.sharding import PartitionSpec as P

HQ = 64
HK = 8
HD = 128
BLK = 64
N_Z = 8
STEPS = 4
ROWS_DEV = 2
BATCH = 16
QH = HQ // HK
HEAD_W = QH * HD
FRESH_W = HEAD_W + 2 * HD
XY = ("x", "y")
GXY = ("g", "x", "y")
NEG = -1e30
LOG2E = 1.4426950408889634
COEF = HD ** (-0.5) * LOG2E


def dot_nt(a, b):
    return lax.dot_general(a, b, (((1,), (1,)), ((), ())), preferred_element_type=jnp.float32)


def dot_nn(a, b):
    return lax.dot_general(a, b, (((1,), (0,)), ((), ())), preferred_element_type=jnp.float32)


def lane_groups(x):
    return [x[:, k * 128 : (k + 1) * 128] for k in range(x.shape[1] // 128)]


def fold(op, x):
    parts = lane_groups(x)
    while len(parts) > 1:
        parts = [op(parts[k], parts[k + 1]) for k in range(0, len(parts) - 1, 2)] + (
            [parts[-1]] if len(parts) % 2 else []
        )
    return parts[0]


def split_scaled(q):
    x = q.astype(jnp.float32) * COEF
    high = x.astype(jnp.bfloat16)
    return jnp.concatenate([high, (x - high.astype(jnp.float32)).astype(jnp.bfloat16)], axis=1)


def score(q2, k):
    return dot_nt(q2, jnp.concatenate([k, k], axis=1))


def softmax_step(s, m_old, acc_old, v):
    top = jnp.max(fold(jnp.maximum, s), axis=1, keepdims=True)
    m_new = jnp.broadcast_to(top, (s.shape[0], 128)) if m_old is None else jnp.maximum(m_old, top)
    w = jnp.concatenate([jnp.exp2(part - m_new) for part in lane_groups(s)], axis=1)
    mixed = dot_nn(w.astype(jnp.bfloat16), jnp.concatenate([v, jnp.ones_like(v)], axis=1))
    if m_old is not None:
        factor = jnp.exp2(m_old - m_new)
        mixed = acc_old * jnp.concatenate([factor, factor], axis=1) + mixed
    return m_new, mixed


def key_slots(segments, z, zs, tok, span):
    width = sum(n for _, _, n in segments)
    col = lax.broadcasted_iota(jnp.int32, (1, span * width), 1)
    at = jnp.zeros((1, span * width), jnp.int32)
    off = 0
    for block in range(span):
        for shift, start, n in segments:
            base = ((z - shift) & (zs - 1)) * tok + block * zs * tok + start - off
            at = jnp.where((col >= off) & (col < off + n), col + base, at)
            off += n
    return at


def joined_blocks(refs, j, span, part):
    return jnp.concatenate([ref[j + i, :, part] for i in range(span) for ref in refs], axis=0)


KEYS = slice(0, HD)
VALUES = slice(HD, 2 * HD)


def prefill_kernel(segments, info, q_ref, *refs):
    n = len(segments)
    kv_refs = refs[:n]
    o_ref, q_s, m_s, acc_s, sa, sb = refs[n:]
    z = info[0]
    length = info[2 + info[1]]
    count, tok, _ = q_ref.shape
    rows = QH * tok
    block = N_Z * tok
    edge = length // block

    def split(p):
        for h in range(QH):
            q_s[p, h * tok : (h + 1) * tok, :] = split_scaled(q_ref[p, :, h * HD : (h + 1) * HD])

    def fill(s_ref, p, j):
        s_ref[...] = score(q_s[p], joined_blocks(kv_refs, j, 1, KEYS))

    def begin(s_ref, p):
        j = jnp.minimum(p, edge)
        at = key_slots(segments, z, N_Z, tok, 1) + j * block
        row = lax.broadcasted_iota(jnp.int32, (rows, 1), 0) % tok
        end = jnp.minimum(p * block + z * tok + row, length - 1)
        s = jnp.where(at <= end, s_ref[...], NEG)
        v = joined_blocks(kv_refs, j, 1, VALUES)
        m_s[p], acc_s[p] = softmax_step(s, None, None, v)

    def take(s_ref, p, j):
        v = joined_blocks(kv_refs, j, 1, VALUES)
        m_s[p], acc_s[p] = softmax_step(s_ref[...], m_s[p], acc_s[p], v)

    def item(t):
        starts = [j * (count - 1) - j * (j - 1) // 2 for j in range(1, count - 1)]
        j = sum((t >= start).astype(jnp.int32) for start in starts)
        p = jnp.minimum(t - j * (count - 1) + j * (j - 1) // 2 + j + 1, count - 1)
        return p, j

    split(0)
    fill(sa, 0, 0)

    def edges(i, carry):
        p = 2 * i
        split(p + 1)
        fill(sb, p + 1, jnp.minimum(p + 1, edge))
        begin(sa, p)
        split(p + 2)
        fill(sa, p + 2, jnp.minimum(p + 2, edge))
        begin(sb, p + 1)
        return carry

    lax.fori_loop(0, count // 2 - 1, edges, 0)
    split(count - 1)
    fill(sb, count - 1, jnp.minimum(count - 1, edge))
    begin(sa, count - 2)
    fill(sa, 1, 0)
    begin(sb, count - 1)

    def body(i, carry):
        fill(sb, *item(2 * i + 1))
        take(sa, *item(2 * i))
        fill(sa, *item(2 * i + 2))
        take(sb, *item(2 * i + 1))
        return carry

    cols = jnp.minimum(edge, count - 1)
    items = (count - 1) * cols - cols * (cols - 1) // 2
    lax.fori_loop(0, items // 2, body, 0)

    @pl.when(items % 2 == 1)
    def _():
        take(sa, *item(items - 1))

    def finish(p, carry):
        out = (acc_s[p, :, :HD] / acc_s[p, :, HD:]).astype(o_ref.dtype)
        for h in range(QH):
            o_ref[p, :, h * HD : (h + 1) * HD] = out[h * tok : (h + 1) * tok, :]
        return carry

    lax.fori_loop(0, count, finish, 0)


def whole(shape):
    return pl.BlockSpec(shape, lambda i, info: (0,) * len(shape))


def prefill(info, q, kvs, segments):
    n, tok, _ = q.shape
    rows = QH * tok
    return pl.pallas_call(
        functools.partial(prefill_kernel, tuple(segments)),
        out_shape=jax.ShapeDtypeStruct(q.shape, q.dtype),
        grid_spec=pltpu.PrefetchScalarGridSpec(
            num_scalar_prefetch=1,
            grid=(1,),
            in_specs=[whole(a.shape) for a in (q, *kvs)],
            out_specs=whole(q.shape),
            scratch_shapes=[
                pltpu.VMEM((n, rows, 2 * HD), jnp.bfloat16),
                pltpu.VMEM((n, rows, 128), jnp.float32),
                pltpu.VMEM((n, rows, 2 * HD), jnp.float32),
                pltpu.VMEM((rows, N_Z * tok), jnp.float32),
                pltpu.VMEM((rows, N_Z * tok), jnp.float32),
            ],
        ),
        compiler_params=pltpu.CompilerParams(vmem_limit_bytes=24 * 2**20),
        cost_estimate=pl.CostEstimate(
            flops=20 * 10**9, transcendentals=10**7, bytes_accessed=4 * 2**20
        ),
        name="prefill",
    )(info, q, *kvs)


def across(column):
    n = column.shape[0]
    same = lax.broadcasted_iota(jnp.int32, (n, n), 0) == lax.broadcasted_iota(jnp.int32, (n, n), 1)
    return jnp.sum(jnp.where(same, column, 0.0), axis=0, keepdims=True)


def places_of_rows(z, g, length, cells, owner, cached):
    total = owner.shape[1]
    limit = jnp.where(owner == g, jnp.minimum(cached * BLK, length), 0).astype(jnp.float32)
    cell = lax.broadcasted_iota(jnp.int32, (cells, 1), 0)
    local = ROWS_DEV * STEPS
    row = cell // local * (ROWS_DEV * N_Z) + z * ROWS_DEV + cell % local // STEPS
    mine = lax.broadcasted_iota(jnp.int32, (cells, total), 1) == row
    held = jnp.sum(jnp.where(mine, limit, 0.0), axis=1, keepdims=True)
    other = across(held)
    before = lax.broadcasted_iota(jnp.int32, (1, cells), 1) // STEPS < cell // STEPS
    ahead = (other > held) | ((other == held) & before)
    place = jnp.sum(jnp.where(ahead, 1.0, 0.0), axis=1, keepdims=True)
    return held, place + (cell % STEPS).astype(jnp.float32)


def verify_kernel(segments, info, x_ref, held_ref, *refs):
    n = len(segments)
    kv_refs = refs[:n]
    o_ref, x_s, lim_s, o_s, q_s, m_s, acc_s, sa, sb = refs[n:]
    z = info[0]
    g = info[1]
    length = info[2 + g]
    cells = x_ref.shape[0] * x_ref.shape[1]
    blocks, tok, _ = kv_refs[0].shape
    width = N_Z * tok
    cut = BATCH * STEPS
    rows = QH * cut
    held, place_col = places_of_rows(z, g, length, cells, held_ref[0:1], held_ref[1:2])
    index = lax.broadcasted_iota(jnp.int32, (cells, cells), 0).astype(jnp.float32)
    pick = index == across(place_col)
    x = x_ref[...].reshape(cells, FRESH_W)
    x_s[...] = dot_nn(jnp.where(pick, 1.0, 0.0).astype(jnp.bfloat16), x).astype(jnp.bfloat16)
    limits = jnp.sum(jnp.where(pick, across(held), 0.0), axis=1, keepdims=True)
    lim_s[...] = jnp.broadcast_to(limits, (cells, 128))
    o_s[...] = jnp.zeros((cells, HEAD_W), jnp.bfloat16)
    places = lane_groups(key_slots(segments, z, N_Z, tok, 1).astype(jnp.float32))

    def batch(b, carry):
        at = pl.ds(pl.multiple_of(b * cut, cut), cut)
        for h in range(QH):
            q_s[h * cut : (h + 1) * cut, :] = split_scaled(x_s[at, h * HD : (h + 1) * HD])
        near = pl.ds(pl.multiple_of(b * cut // 128 * 128, 128), 128)
        col = lax.broadcasted_iota(jnp.int32, (1, 128), 1) - b * cut % 128
        row = lax.broadcasted_iota(jnp.int32, (rows, 1), 0) % cut
        seen = (col <= row) & (col >= row - row % STEPS)
        s = jnp.where(seen, score(q_s[...], x_s[near, HEAD_W : HEAD_W + HD]), NEG)
        m_s[...], acc_s[...] = softmax_step(s, None, None, x_s[near, HEAD_W + HD :])

        def fill(s_ref, j):
            k = joined_blocks(kv_refs, jnp.minimum(j, blocks - 1), 1, KEYS)
            s_ref[...] = score(q_s[...], k)

        def take(s_ref, j):
            left = jnp.concatenate([lim_s[at, :]] * QH, axis=0)
            left = left - (j * width).astype(jnp.float32)
            parts = [
                jnp.where(place < left, part, NEG)
                for place, part in zip(places, lane_groups(s_ref[...]))
            ]
            s = jnp.concatenate(parts, axis=1)
            v = joined_blocks(kv_refs, j, 1, VALUES)
            m_s[...], acc_s[...] = softmax_step(s, m_s[...], acc_s[...], v)

        most = jnp.max(lim_s[at, :]).astype(jnp.int32)
        count = (most + width - 1) // width
        fill(sa, 0)

        def body(i, carry):
            fill(sb, 2 * i + 1)
            take(sa, 2 * i)
            fill(sa, 2 * i + 2)
            take(sb, 2 * i + 1)
            return carry

        lax.fori_loop(0, count // 2, body, 0)

        @pl.when(count % 2 == 1)
        def _():
            take(sa, count - 1)

        out = (acc_s[:, :HD] / acc_s[:, HD:]).astype(jnp.bfloat16)
        for h in range(QH):
            o_s[at, h * HD : (h + 1) * HD] = out[h * cut : (h + 1) * cut, :]
        return carry

    owned = jnp.sum(jnp.where(held > 0.0, 1.0, 0.0)).astype(jnp.int32)
    lax.fori_loop(0, (owned + cut - 1) // cut, batch, 0)
    index = lax.broadcasted_iota(jnp.int32, (cells, cells), 1).astype(jnp.float32)
    put = (index == place_col) & (held > 0.0)
    out = dot_nn(jnp.where(put, 1.0, 0.0).astype(jnp.bfloat16), o_s[...]).astype(jnp.bfloat16)
    o_ref[...] = out.reshape(o_ref.shape)


def verify(info, x, held, kvs, segments):
    cells = x.shape[0] * x.shape[1]
    rows = QH * BATCH * STEPS
    width = N_Z * kvs[0].shape[1]
    operands = (x, held, *kvs)
    out = jax.ShapeDtypeStruct((*x.shape[:2], HEAD_W), x.dtype)
    return pl.pallas_call(
        functools.partial(verify_kernel, tuple(segments)),
        out_shape=out,
        grid_spec=pltpu.PrefetchScalarGridSpec(
            num_scalar_prefetch=1,
            grid=(1,),
            in_specs=[whole(a.shape) for a in operands],
            out_specs=whole(out.shape),
            scratch_shapes=[
                pltpu.VMEM((cells, FRESH_W), jnp.bfloat16),
                pltpu.VMEM((cells, 128), jnp.float32),
                pltpu.VMEM((cells, HEAD_W), jnp.bfloat16),
                pltpu.VMEM((rows, 2 * HD), jnp.bfloat16),
                pltpu.VMEM((rows, 128), jnp.float32),
                pltpu.VMEM((rows, 2 * HD), jnp.float32),
                pltpu.VMEM((rows, width), jnp.float32),
                pltpu.VMEM((rows, width), jnp.float32),
            ],
        ),
        compiler_params=pltpu.CompilerParams(vmem_limit_bytes=24 * 2**20),
        cost_estimate=pl.CostEstimate(
            flops=4 * 10**9, transcendentals=10**6, bytes_accessed=4 * 2**20
        ),
        name="verify",
    )(info, *operands)


def pack_kv_kernel(k_ref, v_ref, o_ref):
    for h in range(HK):
        o_ref[h, :, :HD] = k_ref[0, :, h * HD : (h + 1) * HD]
        o_ref[h, :, HD:] = v_ref[0, :, h * HD : (h + 1) * HD]


def pack_kv(k, v):
    tok = k.shape[1]
    return pl.pallas_call(
        pack_kv_kernel,
        out_shape=jax.ShapeDtypeStruct((HK, tok, 2 * HD), k.dtype),
        name="pack_kv",
    )(k, v)


def pack_q_kernel(x_ref, o_ref):
    for h in range(HK):
        o_ref[h] = x_ref[0, :, h * HEAD_W : (h + 1) * HEAD_W]


def pack_q(q):
    return pl.pallas_call(
        pack_q_kernel,
        out_shape=jax.ShapeDtypeStruct((HK, q.shape[1], HEAD_W), q.dtype),
        compiler_params=pltpu.CompilerParams(vmem_limit_bytes=8 * 2**20),
        name="pack_q",
    )(q)


def unpack_o_kernel(x_ref, o_ref):
    for h in range(HK):
        o_ref[0, :, h * HEAD_W : (h + 1) * HEAD_W] = x_ref[h]


def unpack_o(o):
    return pl.pallas_call(
        unpack_o_kernel,
        out_shape=jax.ShapeDtypeStruct((1, o.shape[1], HK * HEAD_W), o.dtype),
        compiler_params=pltpu.CompilerParams(vmem_limit_bytes=8 * 2**20),
        name="unpack_o",
    )(o)


def pack_rows_kernel(q_ref, k_ref, v_ref, o_ref):
    groups = o_ref.shape[0] // HK

    def joined(ref, at):
        return jnp.concatenate(
            [ref[i, :, at].astype(jnp.float32) for i in range(ref.shape[0])], axis=0
        ).astype(o_ref.dtype)

    for h in range(HK):
        q = joined(q_ref, slice(h * HEAD_W, (h + 1) * HEAD_W))
        k = joined(k_ref, slice(h * HD, (h + 1) * HD))
        v = joined(v_ref, slice(h * HD, (h + 1) * HD))
        for g in range(groups):
            o_ref[g * HK + h, :, :HEAD_W] = q
            o_ref[g * HK + h, :, HEAD_W : HEAD_W + HD] = k
            o_ref[g * HK + h, :, HEAD_W + HD :] = v


def pack_rows(q, k, v, groups):
    return pl.pallas_call(
        pack_rows_kernel,
        out_shape=jax.ShapeDtypeStruct((groups * HK, q.shape[0] * q.shape[1], FRESH_W), q.dtype),
        compiler_params=pltpu.CompilerParams(vmem_limit_bytes=8 * 2**20),
        name="pack_rows",
    )(q, k, v)


def sum_rows_kernel(x_ref, o_ref):
    groups = x_ref.shape[0] // HK
    steps = o_ref.shape[1]
    for h in range(HK):
        total = x_ref[h].astype(jnp.float32)
        for g in range(1, groups):
            total = total + x_ref[g * HK + h].astype(jnp.float32)
        for i in range(o_ref.shape[0]):
            o_ref[i, :, h * HEAD_W : (h + 1) * HEAD_W] = total[
                i * steps : (i + 1) * steps, :
            ].astype(o_ref.dtype)


def sum_rows(x, rows, steps):
    return pl.pallas_call(
        sum_rows_kernel,
        out_shape=jax.ShapeDtypeStruct((rows, steps, HK * HEAD_W), x.dtype),
        compiler_params=pltpu.CompilerParams(vmem_limit_bytes=8 * 2**20),
        name="sum_rows",
    )(x)


def per_device(
    prefill_query,
    prefill_key,
    prefill_value,
    lengths,
    verify_query,
    verify_key,
    verify_value,
    owner,
    cached,
):
    groups = lax.axis_size("g")
    zs = lax.axis_size("z")
    g = lax.axis_index("g")
    z = lax.axis_index("z")
    rows, steps, _ = verify_query.shape
    tok = prefill_query.shape[1]
    half = tok // 2

    def along(array, shift):
        return lax.ppermute(array, "z", [(i, (i + shift) % zs) for i in range(zs)])

    def exchange(array, axes):
        return lax.all_to_all(array, axes, 0, 0, tiled=True)

    own = exchange(pack_kv(prefill_key, prefill_value), XY)
    q_in = pack_q(prefill_query)
    x_in = pack_rows(verify_query, verify_key, verify_value, groups)
    up1, down1 = along(own, 1), along(own, -1)
    q = exchange(q_in, XY)
    up2, down2 = along(up1, 1), along(down1, -1)
    up4 = along(up1[:, :half], 3)
    down4 = along(down1[:, half:], -3)
    up3, down3 = along(up2, 1), along(down2, -1)
    x = exchange(x_in, GXY)
    kvs = [own, up1, down1, up2, down2, up3, down3, up4, down4]
    segments = [(s, 0, tok) for s in (0, 1, -1, 2, -2, 3, -3)]
    segments += [(4, 0, half), (4, half, half)]

    info = jnp.concatenate([jnp.stack([z, g]), lengths]).astype(jnp.int32)
    held = jnp.stack([owner, cached])
    out = prefill(info, q, kvs, segments)
    out = exchange(out, XY)
    decoded = verify(info, x, held, kvs, segments)
    returned = exchange(decoded, GXY)
    return unpack_o(out), sum_rows(returned, rows, steps)


def solution(mesh):
    split = Mesh(mesh.devices.reshape(4, 2, 4, N_Z), ("g", "x", "y", "z"))
    token = P("g", ("x", "y", "z"), None)
    row = P(("g", "x", "y", "z"), None, None)
    return jax.shard_map(
        per_device,
        mesh=split,
        in_specs=(token, token, token, P(), row, row, row, P(), P()),
        out_specs=(token, row),
        check_vma=False,
    )
```

```python
import functools

import jax
import jax.numpy as jnp
from jax import lax
from jax.experimental import pallas as pl
from jax.experimental.pallas import tpu as pltpu
from jax.sharding import Mesh
from jax.sharding import PartitionSpec as P

HQ = 64
HK = 8
HD = 128
BLK = 64
N_Z = 8
STEPS = 4
ROWS_DEV = 2
BATCH = 16
QH = HQ // HK
HEAD_W = QH * HD
FRESH_W = HEAD_W + 2 * HD
XY = ("x", "y")
GXY = ("g", "x", "y")
NEG = -1e30
LOG2E = 1.4426950408889634
COEF = HD ** (-0.5) * LOG2E


def dot_nt(a, b):
    return lax.dot_general(a, b, (((1,), (1,)), ((), ())), preferred_element_type=jnp.float32)


def dot_nn(a, b):
    return lax.dot_general(a, b, (((1,), (0,)), ((), ())), preferred_element_type=jnp.float32)


def lane_groups(x):
    return [x[:, k * 128 : (k + 1) * 128] for k in range(x.shape[1] // 128)]


def fold(op, x):
    parts = lane_groups(x)
    while len(parts) > 1:
        parts = [op(parts[k], parts[k + 1]) for k in range(0, len(parts) - 1, 2)] + (
            [parts[-1]] if len(parts) % 2 else []
        )
    return parts[0]


def split_scaled(q):
    x = q.astype(jnp.float32) * COEF
    high = x.astype(jnp.bfloat16)
    return jnp.concatenate([high, (x - high.astype(jnp.float32)).astype(jnp.bfloat16)], axis=1)


def score(q2, k):
    return dot_nt(q2, jnp.concatenate([k, k], axis=1))


def softmax_step(s, m_old, acc_old, v):
    top = jnp.max(fold(jnp.maximum, s), axis=1, keepdims=True)
    m_new = jnp.broadcast_to(top, (s.shape[0], 128)) if m_old is None else jnp.maximum(m_old, top)
    w = jnp.concatenate([jnp.exp2(part - m_new) for part in lane_groups(s)], axis=1)
    mixed = dot_nn(w.astype(jnp.bfloat16), jnp.concatenate([v, jnp.ones_like(v)], axis=1))
    if m_old is not None:
        factor = jnp.exp2(m_old - m_new)
        mixed = acc_old * jnp.concatenate([factor, factor], axis=1) + mixed
    return m_new, mixed


def key_slots(segments, z, zs, tok, span):
    width = sum(n for _, _, n in segments)
    col = lax.broadcasted_iota(jnp.int32, (1, span * width), 1)
    at = jnp.zeros((1, span * width), jnp.int32)
    off = 0
    for block in range(span):
        for shift, start, n in segments:
            base = ((z - shift) & (zs - 1)) * tok + block * zs * tok + start - off
            at = jnp.where((col >= off) & (col < off + n), col + base, at)
            off += n
    return at


def joined_blocks(refs, j, span, part):
    return jnp.concatenate([ref[j + i, :, part] for i in range(span) for ref in refs], axis=0)


KEYS = slice(0, HD)
VALUES = slice(HD, 2 * HD)


def prefill_kernel(segments, info, q_ref, *refs):
    n = len(segments)
    kv_refs = refs[:n]
    o_ref, q_s, m_s, acc_s, sa, sb = refs[n:]
    z = info[0]
    length = info[2 + info[1]]
    count, tok, _ = q_ref.shape
    rows = QH * tok
    block = N_Z * tok
    edge = length // block

    def split(p):
        for h in range(QH):
            q_s[p, h * tok : (h + 1) * tok, :] = split_scaled(q_ref[p, :, h * HD : (h + 1) * HD])

    def fill(s_ref, p, j):
        s_ref[...] = score(q_s[p], joined_blocks(kv_refs, j, 1, KEYS))

    def begin(s_ref, p):
        j = jnp.minimum(p, edge)
        at = key_slots(segments, z, N_Z, tok, 1) + j * block
        row = lax.broadcasted_iota(jnp.int32, (rows, 1), 0) % tok
        end = jnp.minimum(p * block + z * tok + row, length - 1)
        s = jnp.where(at <= end, s_ref[...], NEG)
        v = joined_blocks(kv_refs, j, 1, VALUES)
        m_s[p], acc_s[p] = softmax_step(s, None, None, v)

    def take(s_ref, p, j):
        v = joined_blocks(kv_refs, j, 1, VALUES)
        m_s[p], acc_s[p] = softmax_step(s_ref[...], m_s[p], acc_s[p], v)

    def item(t):
        starts = [j * (count - 1) - j * (j - 1) // 2 for j in range(1, count - 1)]
        j = sum((t >= start).astype(jnp.int32) for start in starts)
        p = jnp.minimum(t - j * (count - 1) + j * (j - 1) // 2 + j + 1, count - 1)
        return p, j

    split(0)
    fill(sa, 0, 0)

    for p in range(0, count - 2, 2):
        split(p + 1)
        fill(sb, p + 1, jnp.minimum(p + 1, edge))
        begin(sa, p)
        split(p + 2)
        fill(sa, p + 2, jnp.minimum(p + 2, edge))
        begin(sb, p + 1)
    split(count - 1)
    fill(sb, count - 1, jnp.minimum(count - 1, edge))
    begin(sa, count - 2)
    fill(sa, 1, 0)
    begin(sb, count - 1)

    def two(t):
        fill(sb, *item(t + 1))
        take(sa, *item(t))
        fill(sa, *item(t + 2))
        take(sb, *item(t + 1))

    def body(i, carry):
        two(4 * i)
        two(4 * i + 2)
        return carry

    cols = jnp.minimum(edge, count - 1)
    items = (count - 1) * cols - cols * (cols - 1) // 2
    lax.fori_loop(0, items // 4, body, 0)

    @pl.when(items % 4 >= 2)
    def _():
        two(items // 4 * 4)

    @pl.when(items % 2 == 1)
    def _():
        take(sa, *item(items - 1))

    def finish(p, carry):
        out = (acc_s[p, :, :HD] / acc_s[p, :, HD:]).astype(o_ref.dtype)
        for h in range(QH):
            o_ref[p, :, h * HD : (h + 1) * HD] = out[h * tok : (h + 1) * tok, :]
        return carry

    lax.fori_loop(0, count, finish, 0)


def whole(shape):
    return pl.BlockSpec(shape, lambda i, info: (0,) * len(shape))


def prefill(info, q, kvs, segments):
    n, tok, _ = q.shape
    rows = QH * tok
    return pl.pallas_call(
        functools.partial(prefill_kernel, tuple(segments)),
        out_shape=jax.ShapeDtypeStruct(q.shape, q.dtype),
        grid_spec=pltpu.PrefetchScalarGridSpec(
            num_scalar_prefetch=1,
            grid=(1,),
            in_specs=[whole(a.shape) for a in (q, *kvs)],
            out_specs=whole(q.shape),
            scratch_shapes=[
                pltpu.VMEM((n, rows, 2 * HD), jnp.bfloat16),
                pltpu.VMEM((n, rows, 128), jnp.float32),
                pltpu.VMEM((n, rows, 2 * HD), jnp.float32),
                pltpu.VMEM((rows, N_Z * tok), jnp.float32),
                pltpu.VMEM((rows, N_Z * tok), jnp.float32),
            ],
        ),
        compiler_params=pltpu.CompilerParams(vmem_limit_bytes=24 * 2**20),
        cost_estimate=pl.CostEstimate(
            flops=20 * 10**9, transcendentals=10**7, bytes_accessed=4 * 2**20
        ),
        name="prefill",
    )(info, q, *kvs)


def across(column):
    n = column.shape[0]
    same = lax.broadcasted_iota(jnp.int32, (n, n), 0) == lax.broadcasted_iota(jnp.int32, (n, n), 1)
    return jnp.sum(jnp.where(same, column, 0.0), axis=0, keepdims=True)


def places_of_rows(z, g, length, cells, owner, cached):
    total = owner.shape[1]
    limit = jnp.where(owner == g, jnp.minimum(cached * BLK, length), 0).astype(jnp.float32)
    cell = lax.broadcasted_iota(jnp.int32, (cells, 1), 0)
    local = ROWS_DEV * STEPS
    row = cell // local * (ROWS_DEV * N_Z) + z * ROWS_DEV + cell % local // STEPS
    mine = lax.broadcasted_iota(jnp.int32, (cells, total), 1) == row
    held = jnp.sum(jnp.where(mine, limit, 0.0), axis=1, keepdims=True)
    other = across(held)
    before = lax.broadcasted_iota(jnp.int32, (1, cells), 1) // STEPS < cell // STEPS
    ahead = (other > held) | ((other == held) & before)
    place = jnp.sum(jnp.where(ahead, 1.0, 0.0), axis=1, keepdims=True)
    return held, place + (cell % STEPS).astype(jnp.float32)


def sort_kernel(info, x_ref, held_ref, x_out, lim_out, place_out):
    g = info[1]
    cells = x_ref.shape[0] * x_ref.shape[1]
    held, place_col = places_of_rows(
        info[0], g, info[2 + g], cells, held_ref[0:1], held_ref[1:2]
    )
    index = lax.broadcasted_iota(jnp.int32, (cells, cells), 0).astype(jnp.float32)
    pick = index == across(place_col)
    x = x_ref[...].reshape(cells, FRESH_W)
    x_out[...] = dot_nn(jnp.where(pick, 1.0, 0.0).astype(jnp.bfloat16), x).astype(jnp.bfloat16)
    limits = jnp.sum(jnp.where(pick, across(held), 0.0), axis=1, keepdims=True)
    lim_out[...] = jnp.broadcast_to(limits, (cells, 128))
    place = jnp.where(held > 0.0, place_col, -1.0)
    place_out[...] = jnp.broadcast_to(place, (cells, 128))


def sort_rows(info, x, held):
    cells = x.shape[0] * x.shape[1]
    outs = (
        jax.ShapeDtypeStruct((cells, FRESH_W), x.dtype),
        jax.ShapeDtypeStruct((cells, 128), jnp.float32),
        jax.ShapeDtypeStruct((cells, 128), jnp.float32),
    )
    return pl.pallas_call(
        sort_kernel,
        out_shape=outs,
        grid_spec=pltpu.PrefetchScalarGridSpec(
            num_scalar_prefetch=1,
            grid=(1,),
            in_specs=[whole(a.shape) for a in (x, held)],
            out_specs=tuple(whole(a.shape) for a in outs),
        ),
        compiler_params=pltpu.CompilerParams(vmem_limit_bytes=16 * 2**20),
        name="sort_rows",
    )(info, x, held)


def verify_kernel(segments, info, x_s, lim_s, place_ref, *refs):
    n = len(segments)
    kv_refs = refs[:n]
    o_ref, o_s, q_s, m_s, acc_s, sa, sb = refs[n:]
    z = info[0]
    cells = x_s.shape[0]
    blocks, tok, _ = kv_refs[0].shape
    width = N_Z * tok
    cut = BATCH * STEPS
    rows = QH * cut
    o_s[...] = jnp.zeros((cells, HEAD_W), jnp.bfloat16)
    places = lane_groups(key_slots(segments, z, N_Z, tok, 1).astype(jnp.float32))

    def batch(b, carry):
        at = pl.ds(pl.multiple_of(b * cut, cut), cut)
        for h in range(QH):
            q_s[h * cut : (h + 1) * cut, :] = split_scaled(x_s[at, h * HD : (h + 1) * HD])
        near = pl.ds(pl.multiple_of(b * cut // 128 * 128, 128), 128)
        col = lax.broadcasted_iota(jnp.int32, (1, 128), 1) - b * cut % 128
        row = lax.broadcasted_iota(jnp.int32, (rows, 1), 0) % cut
        seen = (col <= row) & (col >= row - row % STEPS)
        s = jnp.where(seen, score(q_s[...], x_s[near, HEAD_W : HEAD_W + HD]), NEG)
        m_s[...], acc_s[...] = softmax_step(s, None, None, x_s[near, HEAD_W + HD :])

        def fill(s_ref, j):
            k = joined_blocks(kv_refs, jnp.minimum(j, blocks - 1), 1, KEYS)
            s_ref[...] = score(q_s[...], k)

        def take(s_ref, j):
            left = jnp.concatenate([lim_s[at, :]] * QH, axis=0)
            left = left - (j * width).astype(jnp.float32)
            parts = [
                jnp.where(place < left, part, NEG)
                for place, part in zip(places, lane_groups(s_ref[...]))
            ]
            s = jnp.concatenate(parts, axis=1)
            v = joined_blocks(kv_refs, j, 1, VALUES)
            m_s[...], acc_s[...] = softmax_step(s, m_s[...], acc_s[...], v)

        most = jnp.max(lim_s[at, :]).astype(jnp.int32)
        count = (most + width - 1) // width
        fill(sa, 0)

        def two(j):
            fill(sb, j + 1)
            take(sa, j)
            fill(sa, j + 2)
            take(sb, j + 1)

        def body(i, carry):
            two(4 * i)
            two(4 * i + 2)
            return carry

        lax.fori_loop(0, count // 4, body, 0)

        @pl.when(count % 4 >= 2)
        def _():
            two(count // 4 * 4)

        @pl.when(count % 2 == 1)
        def _():
            take(sa, count - 1)

        out = (acc_s[:, :HD] / acc_s[:, HD:]).astype(jnp.bfloat16)
        for h in range(QH):
            o_s[at, h * HD : (h + 1) * HD] = out[h * cut : (h + 1) * cut, :]
        return carry

    place = place_ref[:, 0:1]
    owned = jnp.max(place_ref[...]).astype(jnp.int32) + 1
    lax.fori_loop(0, (owned + cut - 1) // cut, batch, 0)
    put = lax.broadcasted_iota(jnp.int32, (cells, cells), 1).astype(jnp.float32) == place
    out = dot_nn(jnp.where(put, 1.0, 0.0).astype(jnp.bfloat16), o_s[...]).astype(jnp.bfloat16)
    o_ref[...] = out.reshape(o_ref.shape)


def verify(info, rows_in, shape, kvs, segments):
    cells = rows_in[0].shape[0]
    rows = QH * BATCH * STEPS
    width = N_Z * kvs[0].shape[1]
    operands = (*rows_in, *kvs)
    out = jax.ShapeDtypeStruct((*shape[:2], HEAD_W), kvs[0].dtype)
    return pl.pallas_call(
        functools.partial(verify_kernel, tuple(segments)),
        out_shape=out,
        grid_spec=pltpu.PrefetchScalarGridSpec(
            num_scalar_prefetch=1,
            grid=(1,),
            in_specs=[whole(a.shape) for a in operands],
            out_specs=whole(out.shape),
            scratch_shapes=[
                pltpu.VMEM((cells, HEAD_W), jnp.bfloat16),
                pltpu.VMEM((rows, 2 * HD), jnp.bfloat16),
                pltpu.VMEM((rows, 128), jnp.float32),
                pltpu.VMEM((rows, 2 * HD), jnp.float32),
                pltpu.VMEM((rows, width), jnp.float32),
                pltpu.VMEM((rows, width), jnp.float32),
            ],
        ),
        compiler_params=pltpu.CompilerParams(vmem_limit_bytes=24 * 2**20),
        cost_estimate=pl.CostEstimate(
            flops=4 * 10**9, transcendentals=10**6, bytes_accessed=4 * 2**20
        ),
        name="verify",
    )(info, *operands)


def pack_kv_kernel(k_ref, v_ref, o_ref):
    for h in range(HK):
        o_ref[h, :, :HD] = k_ref[0, :, h * HD : (h + 1) * HD]
        o_ref[h, :, HD:] = v_ref[0, :, h * HD : (h + 1) * HD]


def pack_kv(k, v):
    tok = k.shape[1]
    return pl.pallas_call(
        pack_kv_kernel,
        out_shape=jax.ShapeDtypeStruct((HK, tok, 2 * HD), k.dtype),
        name="pack_kv",
    )(k, v)


def pack_q_kernel(x_ref, o_ref):
    for h in range(HK):
        o_ref[h] = x_ref[0, :, h * HEAD_W : (h + 1) * HEAD_W]


def pack_q(q):
    return pl.pallas_call(
        pack_q_kernel,
        out_shape=jax.ShapeDtypeStruct((HK, q.shape[1], HEAD_W), q.dtype),
        compiler_params=pltpu.CompilerParams(vmem_limit_bytes=8 * 2**20),
        name="pack_q",
    )(q)


def unpack_o_kernel(x_ref, o_ref):
    for h in range(HK):
        o_ref[0, :, h * HEAD_W : (h + 1) * HEAD_W] = x_ref[h]


def unpack_o(o):
    return pl.pallas_call(
        unpack_o_kernel,
        out_shape=jax.ShapeDtypeStruct((1, o.shape[1], HK * HEAD_W), o.dtype),
        compiler_params=pltpu.CompilerParams(vmem_limit_bytes=8 * 2**20),
        name="unpack_o",
    )(o)


def pack_rows_kernel(q_ref, k_ref, v_ref, o_ref):
    groups = o_ref.shape[0] // HK

    def joined(ref, at):
        return jnp.concatenate(
            [ref[i, :, at].astype(jnp.float32) for i in range(ref.shape[0])], axis=0
        ).astype(o_ref.dtype)

    for h in range(HK):
        q = joined(q_ref, slice(h * HEAD_W, (h + 1) * HEAD_W))
        k = joined(k_ref, slice(h * HD, (h + 1) * HD))
        v = joined(v_ref, slice(h * HD, (h + 1) * HD))
        for g in range(groups):
            o_ref[g * HK + h, :, :HEAD_W] = q
            o_ref[g * HK + h, :, HEAD_W : HEAD_W + HD] = k
            o_ref[g * HK + h, :, HEAD_W + HD :] = v


def pack_rows(q, k, v, groups):
    return pl.pallas_call(
        pack_rows_kernel,
        out_shape=jax.ShapeDtypeStruct((groups * HK, q.shape[0] * q.shape[1], FRESH_W), q.dtype),
        compiler_params=pltpu.CompilerParams(vmem_limit_bytes=8 * 2**20),
        name="pack_rows",
    )(q, k, v)


def sum_rows_kernel(x_ref, o_ref):
    groups = x_ref.shape[0] // HK
    steps = o_ref.shape[1]
    for h in range(HK):
        total = x_ref[h].astype(jnp.float32)
        for g in range(1, groups):
            total = total + x_ref[g * HK + h].astype(jnp.float32)
        for i in range(o_ref.shape[0]):
            o_ref[i, :, h * HEAD_W : (h + 1) * HEAD_W] = total[
                i * steps : (i + 1) * steps, :
            ].astype(o_ref.dtype)


def sum_rows(x, rows, steps):
    return pl.pallas_call(
        sum_rows_kernel,
        out_shape=jax.ShapeDtypeStruct((rows, steps, HK * HEAD_W), x.dtype),
        compiler_params=pltpu.CompilerParams(vmem_limit_bytes=8 * 2**20),
        name="sum_rows",
    )(x)


def per_device(
    prefill_query,
    prefill_key,
    prefill_value,
    lengths,
    verify_query,
    verify_key,
    verify_value,
    owner,
    cached,
):
    groups = lax.axis_size("g")
    zs = lax.axis_size("z")
    g = lax.axis_index("g")
    z = lax.axis_index("z")
    rows, steps, _ = verify_query.shape
    tok = prefill_query.shape[1]
    half = tok // 2

    def along(array, shift):
        return lax.ppermute(array, "z", [(i, (i + shift) % zs) for i in range(zs)])

    def exchange(array, axes):
        return lax.all_to_all(array, axes, 0, 0, tiled=True)

    own = exchange(pack_kv(prefill_key, prefill_value), XY)
    q_in = pack_q(prefill_query)
    x_in = pack_rows(verify_query, verify_key, verify_value, groups)
    up1, down1 = along(own, 1), along(own, -1)
    q = exchange(q_in, XY)
    up2, down2 = along(up1, 1), along(down1, -1)
    up4 = along(up1[:, :half], 3)
    down4 = along(down1[:, half:], -3)
    up3, down3 = along(up2, 1), along(down2, -1)
    x = exchange(x_in, GXY)
    kvs = [own, up1, down1, up2, down2, up3, down3, up4, down4]
    segments = [(s, 0, tok) for s in (0, 1, -1, 2, -2, 3, -3)]
    segments += [(4, 0, half), (4, half, half)]

    info = jnp.concatenate([jnp.stack([z, g]), lengths]).astype(jnp.int32)
    held = jnp.stack([owner, cached])
    rows_in = sort_rows(info, x, held)
    out = prefill(info, q, kvs, segments)
    out = exchange(out, XY)
    decoded = verify(info, rows_in, x.shape, kvs, segments)
    returned = exchange(decoded, GXY)
    return unpack_o(out), sum_rows(returned, rows, steps)


def solution(mesh):
    split = Mesh(mesh.devices.reshape(4, 2, 4, N_Z), ("g", "x", "y", "z"))
    token = P("g", ("x", "y", "z"), None)
    row = P(("g", "x", "y", "z"), None, None)
    return jax.shard_map(
        per_device,
        mesh=split,
        in_specs=(token, token, token, P(), row, row, row, P(), P()),
        out_specs=(token, row),
        check_vma=False,
    )
```
